32 devices in a mesh: rep: 4 (over z), fsdp: 8 (over y, x, core).
Axes of the slice: x: 2, y: 2, z: 4, core: 2. Of those that a mesh axis runs over, the one named last changes fastest.
Arguments:
- hidden: bfloat16 [8192, 7168], P(('rep', 'fsdp')), may hold values from -6 to 6
- out_grad: bfloat16 [8192, 2048], P(('rep', 'fsdp')), may hold values from -0.125 to 0.125
- inner_params: float32 [4, 7168, 2048], P('rep', 'fsdp'), may hold values from -0.132 to 0.132
- first_moment: bfloat16 [4, 7168, 2048], P('rep', 'fsdp'), may hold values from -6 to 6
- second_moment: bfloat16 [4, 7168, 2048], P('rep', 'fsdp'), may hold values from 0.049804688 to 2
- outer_params: float32 [7168, 2048], P('fsdp', 'rep'), may hold values from -0.12 to 0.12
- outer_momentum: float32 [7168, 2048], P('fsdp', 'rep'), may hold values from -0.012 to 0.012
Outputs:
- new_params: float32 [7168, 2048], P('fsdp')
- new_momentum: float32 [7168, 2048], P('fsdp', 'rep')
- new_first: bfloat16 [4, 7168, 2048], P('rep', 'fsdp')
- new_second: bfloat16 [4, 7168, 2048], P('rep', 'fsdp')
The draws below stay inside these ranges and needn't reach their ends.
All inputs are finite; a program needn't handle non-finite values.
Results may differ from the reference program's by a relative error of at most 0.009.
Values may be sent and summed in bfloat16 or wider, within the bound.
A program may use at most 192 MiB of HBM per device.

```python
import math
import jax
import jax.numpy as jnp
from jax import lax

FFW = 7168
DW = 2048
TOK_DEV = 256
INNER_STEP = 500
REPLICAS = 4
TOKENS = 8192
N_FSDP = 8


def base_weights(key):
    inner_key = jax.random.fold_in(key, 11)
    values = jax.random.normal(inner_key, (FFW, DW), jnp.float32)
    return jnp.clip(0.02 * values, -0.12, 0.12)


def draw_outer_params(key, part):
    return base_weights(key)


def draw_inner_params(key, part):
    drift_key = jax.random.fold_in(key, 13)
    drift = jax.random.normal(drift_key, (REPLICAS, FFW, DW), jnp.float32)
    drift = jnp.clip(0.002 * drift, -0.012, 0.012)
    return base_weights(key)[None] + drift


def with_spikes(array, stream_key, source, target, shards_of, factor):
    owner, partner = [(jnp.arange(array.shape[dim]) // (array.shape[dim] // shards_of)).reshape([-1 if axis == dim else 1 for axis in range(array.ndim)]) for dim in (source, target)]
    chosen = jax.random.permutation(stream_key, shards_of)[partner]
    strong = (owner == chosen) | (owner == (partner + shards_of // 2) % shards_of)
    return jnp.where(strong, factor * array, array)


def level_of(stream_key, extent, shards, smallest, top_value):
    def one(position, shards_of):
        draws = jax.random.uniform(jax.random.fold_in(jax.random.fold_in(stream_key, 6), position), (shards_of,), jnp.float32, smallest / len(shards), top_value / len(shards))
        return jnp.repeat(jnp.exp(draws), extent[position] // shards_of).reshape((-1,) + (1,) * (len(extent) - position - 1))

    level = one(*shards[0])
    for cut in shards[1:]:
        level = level * one(*cut)
    return level


def noise(own_key, shape, spread, most, cuts=(), kind=jnp.bfloat16):
    values = spread * jax.random.normal(own_key, shape, jnp.float32)
    if cuts:
        values = values * level_of(own_key, shape, cuts, -0.22, 0.18)
    return jnp.clip(values, -most, most).astype(kind)


def bell_draw_with(key, dims, deviation, most, pieces, heavy, held_as=jnp.bfloat16):
    result = deviation * jax.random.normal(key, dims, jnp.float32)
    if pieces:
        result = result * level_of(key, dims, pieces, -0.22, 0.18)
    return jnp.clip(with_spikes(result, jax.random.fold_in(key, 3), *heavy), -most, most).astype(held_as)


def setup_inputs(seed: int = 0) -> dict:
    streams_of = jax.random.split(jax.random.key(seed), 8)
    return {
        "hidden": bell_draw_with(streams_of[0], (TOKENS, FFW), 1.0, 6.0, ((0, 32),), (0, 1, 32, 2.75)),
        "out_grad": noise(streams_of[1], (TOKENS, DW), (TOK_DEV * N_FSDP) ** -0.5, 0.125, ((0, 32),)),
        "inner_params": draw_inner_params(jax.random.fold_in(streams_of[7], 71), 0),
        "first_moment": noise(streams_of[3], (REPLICAS, FFW, DW), 1.0, 6.0, ((0, 4), (1, 8))),
        "second_moment": jnp.clip(jnp.exp(math.log(2.0) - 3.6927934 * jax.random.uniform(streams_of[4], (REPLICAS, FFW, DW), jnp.float32) ** level_of(streams_of[4], (REPLICAS, FFW, DW), ((0, 4), (1, 8)), -0.2, 0.2)), 0.049804688, 2.0).astype(jnp.bfloat16),
        "outer_params": draw_outer_params(jax.random.fold_in(streams_of[7], 71), 0),
        "outer_momentum": noise(streams_of[6], (FFW, DW), 0.002, 0.012, ((0, 8), (1, 4)), jnp.float32),
    }


beta_one = 0.9
beta_two = 0.95
epsilon = 1e-08
inner_rate = 0.0004
weight_decay = 0.1
outer_rate = 0.7
nesterov = 0.9

def add_block(running, block_pair):
    hidden_block, grad_block = block_pair
    partial_value = jnp.dot(hidden_block.T, grad_block, preferred_element_type=jnp.float32)
    rounded = lax.optimization_barrier(partial_value.astype(jnp.bfloat16)).astype(jnp.float32)
    return (running + rounded, None)

def replica_step(running, inputs):
    hidden_blocks, grad_blocks, params, first_state, second = inputs
    gradient, unused = lax.scan(add_block, jnp.zeros((FFW, DW), jnp.float32), (hidden_blocks, grad_blocks))
    moment_one = beta_one * first_state.astype(jnp.float32) + (1.0 - beta_one) * gradient
    moment_two = beta_two * second.astype(jnp.float32) + (1.0 - beta_two) * gradient * gradient
    corrected_one = moment_one / (1.0 - beta_one ** INNER_STEP)
    corrected_two = moment_two / (1.0 - beta_two ** INNER_STEP)
    stepped = params - inner_rate * (corrected_one / (jnp.sqrt(corrected_two) + epsilon) + weight_decay * params)
    return (running + stepped, (moment_one.astype(jnp.bfloat16), moment_two.astype(jnp.bfloat16)))

def reference(hidden, out_grad, inner_params, first_moment, second_moment, outer_params, outer_momentum):
    hidden_blocks = hidden.reshape(REPLICAS, N_FSDP, TOK_DEV, FFW)
    grad_blocks = out_grad.reshape(REPLICAS, N_FSDP, TOK_DEV, DW)
    summed, moments = lax.scan(replica_step, jnp.zeros((FFW, DW), jnp.float32), (hidden_blocks, grad_blocks, inner_params, first_moment, second_moment))
    outer_delta = outer_params - summed / REPLICAS
    new_momentum = nesterov * outer_momentum + outer_delta
    new_params = outer_params - outer_rate * (outer_delta + nesterov * new_momentum)
    return (new_params, new_momentum, moments[0], moments[1])
```

```python
import functools

import jax
import jax.numpy as jnp
from jax import lax
from jax.experimental import pallas as pl
from jax.experimental.pallas import tpu as pltpu
from jax.sharding import PartitionSpec as P

INNER_STEP = 500

beta_one = 0.9
beta_two = 0.95
epsilon = 1e-08
inner_rate = 0.0004
weight_decay = 0.1
outer_rate = 0.7
nesterov = 0.9

WIRE = jnp.bfloat16
WIRE_SCALE = 16.0
LAG_OWN = 2
LAG_FORWARD = 4


def encode(value):
    scaled = value * WIRE_SCALE
    square = scaled * scaled
    fourth = square * square
    eighth = fourth * fourth
    return jnp.where(scaled < 0.0, -eighth, eighth).astype(WIRE)


def decode(coded):
    wide = coded.astype(jnp.float32)
    root = jnp.sqrt(jnp.sqrt(jnp.sqrt(jnp.abs(wide)))) * (1.0 / WIRE_SCALE)
    return jnp.where(wide < 0.0, -root, root)


def outer_kernel(
    n, chunks, step_ref, outer_ref, mom_ref, out_ref, newmom_ref,
    from_left, from_right, acc, total,
    rs_send, rs_left, rs_right, ag_right, ag_left, ag_recv,
):
    z = lax.axis_index("rep")
    rows, block = outer_ref.shape
    rc = rows // chunks
    has_left, has_right = z > 0, z < n - 1

    barrier = pltpu.get_barrier_semaphore()

    @pl.when(has_left)
    def _():
        pl.semaphore_signal(barrier, inc=1, device_id={"rep": z - 1})

    @pl.when(has_right)
    def _():
        pl.semaphore_signal(barrier, inc=1, device_id={"rep": z + 1})

    pl.semaphore_wait(barrier, has_left.astype(jnp.int32) + has_right.astype(jnp.int32))

    def part(c, o):
        start = o * block
        if not isinstance(o, int):
            start = pl.multiple_of(start, 128)
        return pl.ds(pl.multiple_of(c * rc, rc), rc), pl.ds(start, block)

    def send_sum(src, c, o, to_right):
        at = part(c, o)
        return pltpu.make_async_remote_copy(
            src_ref=src.at[at],
            dst_ref=(from_left if to_right else from_right).at[at],
            send_sem=rs_send.at[c, o],
            recv_sem=(rs_left if to_right else rs_right).at[c, o],
            device_id={"rep": z + 1 if to_right else z - 1},
        )

    def send_new(c, o, to_right):
        at = part(c, o)
        return pltpu.make_async_remote_copy(
            src_ref=out_ref.at[at],
            dst_ref=out_ref.at[at],
            send_sem=(ag_right if to_right else ag_left).at[c, o],
            recv_sem=ag_recv.at[c, o],
            device_id={"rep": z + 1 if to_right else z - 1},
        )

    def wave(c, to_right):
        first = z == 0 if to_right else z == n - 1
        order = range(n - 1, 0, -1) if to_right else range(n - 1)
        for o in order:
            beyond = o > z if to_right else o < z
            at = part(c, o)

            @pl.when(jnp.logical_and(beyond, first))
            def _():
                acc[at] = encode(step_ref[at])
                send_sum(acc, c, o, to_right).start()

            @pl.when(jnp.logical_and(beyond, jnp.logical_not(first)))
            def _():
                send_sum(acc, c, o, to_right).wait_recv()
                came = (from_left if to_right else from_right)[at]
                acc[at] = encode(decode(came) + step_ref[at])
                send_sum(acc, c, o, to_right).start()

    def own(c):
        at = part(c, z)
        here = pl.ds(pl.multiple_of(c * rc, rc), rc)
        total[...] = step_ref[at]

        @pl.when(has_left)
        def _():
            send_sum(acc, c, z, True).wait_recv()
            total[...] += decode(from_left[at])

        @pl.when(has_right)
        def _():
            send_sum(acc, c, z, False).wait_recv()
            total[...] += decode(from_right[at])

        delta = outer_ref[here, :] - total[...] / n
        momentum = nesterov * mom_ref[here, :] + delta
        newmom_ref[here, :] = momentum
        updated = outer_ref[here, :] - outer_rate * (delta + nesterov * momentum)
        out_ref[at] = updated.astype(WIRE)

        @pl.when(has_right)
        def _():
            send_new(c, z, True).start()

        @pl.when(has_left)
        def _():
            send_new(c, z, False).start()

    def forward(c):
        for distance in range(1, n):
            for to_right in (True, False):
                o = z - distance if to_right else z + distance
                there = o >= 0 if to_right else o < n

                @pl.when(there)
                def _():
                    send_new(c, o, to_right).wait_recv()

                @pl.when(jnp.logical_and(there, has_right if to_right else has_left))
                def _():
                    send_new(c, o, to_right).start()

    def body(t, carry):
        @pl.when(t < chunks)
        def _():
            near_left = z < n // 2

            @pl.when(near_left)
            def _():
                wave(t, True)
                wave(t, False)

            @pl.when(jnp.logical_not(near_left))
            def _():
                wave(t, False)
                wave(t, True)

        @pl.when(jnp.logical_and(t >= LAG_OWN, t < chunks + LAG_OWN))
        def _():
            own(t - LAG_OWN)

        @pl.when(t >= LAG_FORWARD)
        def _():
            forward(t - LAG_FORWARD)

        return carry

    lax.fori_loop(0, chunks + LAG_FORWARD, body, 0)

    def drain(c, carry):
        for o in range(n):
            @pl.when(o > z)
            def _():
                send_sum(acc, c, o, True).wait_send()

            @pl.when(o < z)
            def _():
                send_sum(acc, c, o, False).wait_send()

            @pl.when(jnp.logical_and(o <= z, has_right))
            def _():
                send_new(c, o, True).wait_send()

            @pl.when(jnp.logical_and(o >= z, has_left))
            def _():
                send_new(c, o, False).wait_send()

        return carry

    lax.fori_loop(0, chunks, drain, 0)


def outer_step(stepped, outer_params, outer_momentum):
    n = lax.axis_size("rep")
    rows, block = outer_params.shape
    chunks = max(c for c in range(1, 15) if rows % (16 * c) == 0)
    vmem = pl.BlockSpec(memory_space=pltpu.VMEM)
    dma = pltpu.SemaphoreType.DMA((chunks, n))
    return pl.pallas_call(
        functools.partial(outer_kernel, n, chunks),
        out_shape=(
            jax.ShapeDtypeStruct(stepped.shape, WIRE),
            jax.ShapeDtypeStruct(outer_params.shape, jnp.float32),
        ),
        in_specs=[vmem] * 3,
        out_specs=(vmem, vmem),
        scratch_shapes=[
            pltpu.VMEM(stepped.shape, WIRE),
            pltpu.VMEM(stepped.shape, WIRE),
            pltpu.VMEM(stepped.shape, WIRE),
            pltpu.VMEM((rows // chunks, block), jnp.float32),
            dma, dma, dma, dma, dma, dma,
        ],
        compiler_params=pltpu.CompilerParams(
            collective_id=0, has_side_effects=True, vmem_limit_bytes=40 * 2**20
        ),
    )(stepped, outer_params, outer_momentum)


def per_device(
    hidden, out_grad, inner_params, first_moment, second_moment, outer_params, outer_momentum
):
    columns = lax.all_to_all(hidden, "fsdp", split_axis=1, concat_axis=0, tiled=True)
    segment = lax.all_gather(out_grad, "fsdp", axis=0, tiled=True)
    token_count = hidden.shape[0]
    blocks = segment.shape[0] // token_count
    gradient = jnp.einsum(
        "btf,btd->fd",
        columns.reshape(blocks, token_count, columns.shape[1]),
        segment.reshape(blocks, token_count, segment.shape[1]),
        preferred_element_type=jnp.float32,
    )
    stacked = gradient[None]
    moment_one = beta_one * first_moment.astype(jnp.float32) + (1.0 - beta_one) * stacked
    moment_two = beta_two * second_moment.astype(jnp.float32) + (1.0 - beta_two) * stacked * stacked
    corrected_one = moment_one / (1.0 - beta_one**INNER_STEP)
    corrected_two = moment_two / (1.0 - beta_two**INNER_STEP)
    stepped = inner_params - inner_rate * (
        corrected_one / (jnp.sqrt(corrected_two) + epsilon) + weight_decay * inner_params
    )
    gathered, new_momentum = outer_step(stepped[0], outer_params, outer_momentum)
    return (
        gathered.astype(jnp.float32),
        new_momentum,
        moment_one.astype(jnp.bfloat16),
        moment_two.astype(jnp.bfloat16),
    )


def solution(mesh):
    return jax.shard_map(
        per_device,
        mesh=mesh,
        in_specs=(
            P(("rep", "fsdp"), None),
            P(("rep", "fsdp"), None),
            P("rep", "fsdp", None),
            P("rep", "fsdp", None),
            P("rep", "fsdp", None),
            P("fsdp", "rep"),
            P("fsdp", "rep"),
        ),
        out_specs=(
            P("fsdp", None),
            P("fsdp", "rep"),
            P("rep", "fsdp", None),
            P("rep", "fsdp", None),
        ),
        check_vma=False,
    )
```

```python
import functools

import jax
import jax.numpy as jnp
from jax import lax
from jax.experimental import pallas as pl
from jax.experimental.pallas import tpu as pltpu
from jax.sharding import PartitionSpec as P

INNER_STEP = 500

beta_one = 0.9
beta_two = 0.95
epsilon = 1e-08
inner_rate = 0.0004
weight_decay = 0.1
outer_rate = 0.7
nesterov = 0.9

WIRE = jnp.bfloat16
WIRE_SCALE = 16.0


def encode(value):
    scaled = value * WIRE_SCALE
    square = scaled * scaled
    fourth = square * square
    eighth = fourth * fourth
    return jnp.where(scaled < 0.0, -eighth, eighth).astype(WIRE)


def decode(coded):
    wide = coded.astype(jnp.float32)
    root = jnp.sqrt(jnp.sqrt(jnp.sqrt(jnp.abs(wide)))) * (1.0 / WIRE_SCALE)
    return jnp.where(wide < 0.0, -root, root)


def outer_kernel(
    n, chunks, step_ref, outer_ref, mom_ref, out_ref, newmom_ref,
    from_left, from_right, acc, total,
    rs_send, rs_left, rs_right, ag_right, ag_left, ag_recv,
):
    z = lax.axis_index("rep")
    rows, block = outer_ref.shape
    rc = rows // chunks
    has_left, has_right = z > 0, z < n - 1

    barrier = pltpu.get_barrier_semaphore()

    @pl.when(has_left)
    def _():
        pl.semaphore_signal(barrier, inc=1, device_id={"rep": z - 1})

    @pl.when(has_right)
    def _():
        pl.semaphore_signal(barrier, inc=1, device_id={"rep": z + 1})

    pl.semaphore_wait(barrier, has_left.astype(jnp.int32) + has_right.astype(jnp.int32))

    def part(c, o):
        start = o * block
        if not isinstance(o, int):
            start = pl.multiple_of(start, 128)
        return pl.ds(pl.multiple_of(c * rc, rc), rc), pl.ds(start, block)

    def send_sum(src, c, o, to_right):
        at = part(c, o)
        return pltpu.make_async_remote_copy(
            src_ref=src.at[at],
            dst_ref=(from_left if to_right else from_right).at[at],
            send_sem=rs_send.at[c, o],
            recv_sem=(rs_left if to_right else rs_right).at[c, o],
            device_id={"rep": z + 1 if to_right else z - 1},
        )

    def send_new(c, o, to_right):
        at = part(c, o)
        return pltpu.make_async_remote_copy(
            src_ref=out_ref.at[at],
            dst_ref=out_ref.at[at],
            send_sem=(ag_right if to_right else ag_left).at[c, o],
            recv_sem=ag_recv.at[c, o],
            device_id={"rep": z + 1 if to_right else z - 1},
        )

    def wave(c, to_right):
        first = z == 0 if to_right else z == n - 1
        order = range(n - 1, 0, -1) if to_right else range(n - 1)
        for o in order:
            beyond = o > z if to_right else o < z
            at = part(c, o)

            @pl.when(jnp.logical_and(beyond, first))
            def _():
                acc[at] = encode(step_ref[at])
                send_sum(acc, c, o, to_right).start()

            @pl.when(jnp.logical_and(beyond, jnp.logical_not(first)))
            def _():
                send_sum(acc, c, o, to_right).wait_recv()
                came = (from_left if to_right else from_right)[at]
                acc[at] = encode(decode(came) + step_ref[at])
                send_sum(acc, c, o, to_right).start()

    def own(c):
        at = part(c, z)
        here = pl.ds(pl.multiple_of(c * rc, rc), rc)
        total[...] = step_ref[at]

        @pl.when(has_left)
        def _():
            send_sum(acc, c, z, True).wait_recv()
            total[...] += decode(from_left[at])

        @pl.when(has_right)
        def _():
            send_sum(acc, c, z, False).wait_recv()
            total[...] += decode(from_right[at])

        delta = outer_ref[here, :] - total[...] / n
        momentum = nesterov * mom_ref[here, :] + delta
        newmom_ref[here, :] = momentum
        updated = outer_ref[here, :] - outer_rate * (delta + nesterov * momentum)
        out_ref[at] = updated.astype(WIRE)

        @pl.when(has_right)
        def _():
            send_new(c, z, True).start()

        @pl.when(has_left)
        def _():
            send_new(c, z, False).start()

    def within(c, work):
        @pl.when(jnp.logical_and(c >= 0, c < chunks))
        def _():
            work(c)

    def own_lag(o):
        return jnp.maximum(o, n - 1 - o)

    def forward(t, distance, to_right):
        o = z - distance if to_right else z + distance
        there = o >= 0 if to_right else o < n
        c = t - own_lag(o) - distance
        ready = jnp.logical_and(there, jnp.logical_and(c >= 0, c < chunks))

        @pl.when(ready)
        def _():
            send_new(c, o, to_right).wait_recv()

        @pl.when(jnp.logical_and(ready, has_right if to_right else has_left))
        def _():
            send_new(c, o, to_right).start()

    def body(t, carry):
        within(t - z, lambda c: wave(c, True))
        within(t - (n - 1 - z), lambda c: wave(c, False))
        within(t - own_lag(z), own)
        for distance in range(1, n):
            forward(t, distance, True)
            forward(t, distance, False)
        return carry

    lax.fori_loop(0, chunks + 2 * (n - 1), body, 0)

    def drain(c, carry):
        for o in range(n):
            @pl.when(o > z)
            def _():
                send_sum(acc, c, o, True).wait_send()

            @pl.when(o < z)
            def _():
                send_sum(acc, c, o, False).wait_send()

            @pl.when(jnp.logical_and(o <= z, has_right))
            def _():
                send_new(c, o, True).wait_send()

            @pl.when(jnp.logical_and(o >= z, has_left))
            def _():
                send_new(c, o, False).wait_send()

        return carry

    lax.fori_loop(0, chunks, drain, 0)


def outer_step(stepped, outer_params, outer_momentum):
    n = lax.axis_size("rep")
    rows, block = outer_params.shape
    chunks = max(c for c in range(1, 15) if rows % (16 * c) == 0)
    vmem = pl.BlockSpec(memory_space=pltpu.VMEM)
    dma = pltpu.SemaphoreType.DMA((chunks, n))
    return pl.pallas_call(
        functools.partial(outer_kernel, n, chunks),
        out_shape=(
            jax.ShapeDtypeStruct(stepped.shape, WIRE),
            jax.ShapeDtypeStruct(outer_params.shape, jnp.float32),
        ),
        in_specs=[vmem] * 3,
        out_specs=(vmem, vmem),
        scratch_shapes=[
            pltpu.VMEM(stepped.shape, WIRE),
            pltpu.VMEM(stepped.shape, WIRE),
            pltpu.VMEM(stepped.shape, WIRE),
            pltpu.VMEM((rows // chunks, block), jnp.float32),
            dma, dma, dma, dma, dma, dma,
        ],
        compiler_params=pltpu.CompilerParams(
            collective_id=0, has_side_effects=True, vmem_limit_bytes=40 * 2**20
        ),
    )(stepped, outer_params, outer_momentum)


def per_device(
    hidden, out_grad, inner_params, first_moment, second_moment, outer_params, outer_momentum
):
    columns = lax.all_to_all(hidden, "fsdp", split_axis=1, concat_axis=0, tiled=True)
    segment = lax.all_gather(out_grad, "fsdp", axis=0, tiled=True)
    token_count = hidden.shape[0]
    blocks = segment.shape[0] // token_count
    gradient = jnp.einsum(
        "btf,btd->fd",
        columns.reshape(blocks, token_count, columns.shape[1]),
        segment.reshape(blocks, token_count, segment.shape[1]),
        preferred_element_type=jnp.float32,
    )
    stacked = gradient[None]
    moment_one = beta_one * first_moment.astype(jnp.float32) + (1.0 - beta_one) * stacked
    moment_two = beta_two * second_moment.astype(jnp.float32) + (1.0 - beta_two) * stacked * stacked
    corrected_one = moment_one / (1.0 - beta_one**INNER_STEP)
    corrected_two = moment_two / (1.0 - beta_two**INNER_STEP)
    stepped = inner_params - inner_rate * (
        corrected_one / (jnp.sqrt(corrected_two) + epsilon) + weight_decay * inner_params
    )
    gathered, new_momentum = outer_step(stepped[0], outer_params, outer_momentum)
    return (
        gathered.astype(jnp.float32),
        new_momentum,
        moment_one.astype(jnp.bfloat16),
        moment_two.astype(jnp.bfloat16),
    )


def solution(mesh):
    return jax.shard_map(
        per_device,
        mesh=mesh,
        in_specs=(
            P(("rep", "fsdp"), None),
            P(("rep", "fsdp"), None),
            P("rep", "fsdp", None),
            P("rep", "fsdp", None),
            P("rep", "fsdp", None),
            P("fsdp", "rep"),
            P("fsdp", "rep"),
        ),
        out_specs=(
            P("fsdp", None),
            P("fsdp", "rep"),
            P("rep", "fsdp", None),
            P("rep", "fsdp", None),
        ),
        check_vma=False,
    )
```
